32 devices in a mesh: blk: 8 (over y, x, core), grp: 4 (over z).
Axes of the slice: x: 2, y: 2, z: 4, core: 2. Of those that a mesh axis runs over, the one named last changes fastest.
Arguments:
- source: float32 [2048, 128], P(('blk', 'grp')), may hold values from -3 to 3
- target: float32 [2048, 128], P(('blk', 'grp')), may hold values from -3 to 3
- source_mass: float32 [2048], P(('blk', 'grp')), may hold values from 0.25 to 4
- target_mass: float32 [2048], P(('blk', 'grp')), may hold values from 0.25 to 4
Outputs:
- source_dual: float32 [2048], P(('blk', 'grp'))
- target_dual: float32 [2048], P(('blk', 'grp'))
The draws below stay inside these ranges and needn't reach their ends.
All inputs are finite; a program needn't handle non-finite values.
Results may differ from the reference program's by a relative error of at most 0.0003.
Values sent between devices are 32-bit elements; how exact they have to be, the bound alone decides.
A program may use at most 64 MiB of HBM per device.

```python
import math
import jax
import jax.numpy as jnp
from jax import lax

D = 128
ITERS = 8
POINTS = 2048


def cloud_parts(key):
    cluster_count = max(POINTS // 64, 1)
    centres = jax.random.normal(jax.random.fold_in(key, 3), (cluster_count, D), jnp.float32)
    member = jax.random.randint(jax.random.fold_in(key, 5), (POINTS,), 0, cluster_count)
    spread = jax.random.normal(jax.random.fold_in(key, 7), (POINTS, D), jnp.float32)
    base = 0.11 * centres[member] + 0.1 * spread
    order = jax.random.permutation(jax.random.fold_in(key, 9), POINTS)
    return (base, order)


def far_shift(key):
    picked_count = max(POINTS // 256, 2)
    picks = jax.random.permutation(jax.random.fold_in(key, 19), POINTS)[:picked_count]
    strength = jax.random.uniform(jax.random.fold_in(key, 23), (picked_count,), jnp.float32, 0.85, 1.25)
    flags = jnp.zeros((POINTS,), jnp.float32).at[picks].set(strength)
    return (110.0 / D) ** 0.5 * flags[:, None]


def draw_source(key, part):
    base, order = cloud_parts(key)
    noise = 0.05 * jax.random.normal(jax.random.fold_in(key, 11), (POINTS, D), jnp.float32)
    points = base + noise
    points = points + far_shift(key)
    return jnp.clip(points, -3.0, 3.0)


def draw_target(key, part):
    base, order = cloud_parts(key)
    matched = base[order]
    noise = 0.05 * jax.random.normal(jax.random.fold_in(key, 13), (POINTS, D), jnp.float32)
    return jnp.clip(matched + noise, -3.0, 3.0)


def levels(key, dims, pieces, least, top_value):
    level, own = 1.0, jax.random.fold_in(key, 6)
    for dim, shards_of in pieces:
        heights = jnp.exp(jax.random.uniform(jax.random.fold_in(own, dim), (shards_of,), jnp.float32, least / len(pieces), top_value / len(pieces)))
        level = level * jnp.repeat(heights, dims[dim] // shards_of).reshape([-1 if axis == dim else 1 for axis in range(len(dims))])
    return level


def setup_inputs(seed: int = 0) -> dict:
    key_of = jax.random.split(jax.random.key(seed), 5)
    source = draw_source(jax.random.fold_in(key_of[4], 71), 0)
    target = draw_target(jax.random.fold_in(key_of[4], 71), 0)
    source_mass = jnp.clip(jnp.exp(math.log(4.0) - 2.7725887 * jax.random.uniform(key_of[2], (POINTS,), jnp.float32) ** levels(key_of[2], (POINTS,), ((0, 32),), -0.2, 0.2)), 0.25, 4.0)
    target_mass = jnp.clip(jnp.exp(math.log(4.0) - 2.7725887 * jax.random.uniform(key_of[3], (POINTS,), jnp.float32) ** levels(key_of[3], (POINTS,), ((0, 32),), -0.2, 0.2)), 0.25, 4.0)
    return {"source": source, "target": target, "source_mass": source_mass, "target_mass": target_mass}


eps = 0.5


def half_step(rows, cols, col_dual, col_logmass):
    total = rows.shape[0]
    width = rows.shape[1]
    block = math.gcd(total, 1024)
    col_sq = jnp.sum(cols * cols, axis=1)

    def one_block(piece):
        row_sq = jnp.sum(piece * piece, axis=1)
        inner = lax.dot_general(piece, cols, (((1,), (1,)), ((), ())), precision=lax.Precision.HIGHEST, preferred_element_type=jnp.float32)
        cost = row_sq[:, None] + col_sq[None, :] - 2.0 * inner
        score = col_logmass[None, :] + (col_dual[None, :] - cost) / eps
        top = jnp.max(score, axis=1)
        total_exp = jnp.sum(jnp.exp(score - top[:, None]), axis=1)
        return -eps * (top + jnp.log(total_exp))

    return lax.map(one_block, rows.reshape(total // block, block, width)).reshape(total)


def reference(source, target, source_mass, target_mass):
    log_source = jnp.log(source_mass)
    log_target = jnp.log(target_mass)
    target_dual = jnp.zeros((target.shape[0],), jnp.float32)
    source_dual = jnp.zeros((source.shape[0],), jnp.float32)
    for step in range(ITERS):
        source_dual = half_step(source, target, target_dual, log_target)
        target_dual = half_step(target, source, source_dual, log_source)
    return source_dual, target_dual
```

```python
import functools
import math

import jax
import jax.numpy as jnp
from jax import lax
from jax.experimental import pallas as pl
from jax.experimental.pallas import tpu as pltpu
from jax.sharding import PartitionSpec as P

ITERS = 8
eps = 0.5
LOG2E = math.log2(math.e)
ALPHA = LOG2E / eps
LANES = 128
SUB = 8
MESH = pl.DeviceIdType.MESH
BUDGET = 36 * 2**20


def exp2(x):
    return jnp.exp2(x)


def log2(x):
    return jnp.log(x) * LOG2E


def lse_blocks(pairs):
    top = functools.reduce(jnp.maximum, [m for m, _ in pairs])
    if len(pairs) == 1:
        return pairs[0]
    return top, sum(s * exp2(m - top) for m, s in pairs)


def kernel(blk_n, grp_n, part, count, src_ref, tgt_ref, smass_ref, tmass_ref, out_ref,
           src_all, tgt_all, spack, tpack, cost, tcat, u, v, loga, logb, part_lse,
           s_send, s_recv, t_send, t_recv, x_send, x_recv):
    n_dev = blk_n * grp_n
    rep = LANES // count
    chunks = n_dev // rep
    quads = blk_n // part
    t_dev = quads * grp_n
    nj = t_dev * count
    b, g = lax.axis_index("blk"), lax.axis_index("grp")
    me = b * grp_n + g
    q, p = b // part, b % part
    mine_t = q * grp_n + g

    barrier = pltpu.get_barrier_semaphore()

    def greet(step, _):
        other = lax.rem(me + step, n_dev)
        pl.semaphore_signal(barrier, inc=1, device_id=(other // grp_n, other % grp_n), device_id_type=MESH)
        return 0

    lax.fori_loop(1, n_dev, greet, 0)

    lane = lax.broadcasted_iota(jnp.int32, (1, LANES), 1)
    here = lane // count == me % rep

    def pack(ref, mass_ref, out, scale):
        out[0:count, :] = ref[...] * scale
        row = log2(mass_ref[...])
        row = jnp.where(here, jnp.concatenate([row] * rep, axis=1), 0.0)
        out[count : count + SUB, :] = jnp.broadcast_to(row, (SUB, LANES))

    pack(src_ref, smass_ref, spack, 2.0 * ALPHA)
    pack(tgt_ref, tmass_ref, tpack, 1.0)
    src_all[pl.ds(me, 1)] = spack[...][None]
    tgt_all[pl.ds(mine_t, 1)] = tpack[...][None]
    pl.semaphore_wait(barrier, n_dev - 1)

    def tgt_copy(slot, r, sem_slot):
        return pltpu.make_async_remote_copy(
            src_ref=tpack, dst_ref=tgt_all.at[slot],
            send_sem=t_send.at[r], recv_sem=t_recv.at[sem_slot],
            device_id=((r // grp_n) * part + p, r % grp_n), device_id_type=MESH)

    def src_copy(slot, d):
        return pltpu.make_async_remote_copy(
            src_ref=spack, dst_ref=src_all.at[slot],
            send_sem=s_send.at[d], recv_sem=s_recv.at[slot],
            device_id=(d // grp_n, d % grp_n), device_id_type=MESH)

    def send_t(step, _):
        r = lax.rem(mine_t + step, t_dev)
        tgt_copy(mine_t, r, mine_t).start()
        return 0

    def send_s(step, _):
        src_copy(me, lax.rem(me + step, n_dev)).start()
        return 0

    def wait_t(step, _):
        r = lax.rem(mine_t + step, t_dev)
        tgt_copy(mine_t, r, mine_t).wait_send()
        tgt_copy(r, r, r).wait_recv()
        return 0

    def wait_s(step, _):
        d = lax.rem(me + step, n_dev)
        src_copy(me, d).wait_send()
        src_copy(d, d).wait_recv()
        return 0

    lax.fori_loop(1, t_dev, send_t, 0)
    lax.fori_loop(1, n_dev, send_s, 0)
    lax.fori_loop(1, t_dev, wait_t, 0)

    eye = (lax.broadcasted_iota(jnp.int32, (count, LANES), 1) % count
           == lax.broadcasted_iota(jnp.int32, (count, LANES), 0))
    for r in range(t_dev):
        rows = slice(r * count, (r + 1) * count)
        block = tgt_all[r, 0:count, :]
        tcat[rows, :] = block
        mass = jnp.sum(jnp.where(eye, tgt_all[r, count : count + 1, :], 0.0), axis=1, keepdims=True)
        square = jnp.sum(block * block, axis=1, keepdims=True)
        logb[rows, :] = jnp.broadcast_to(mass, (count, LANES))
        u[rows, :] = jnp.broadcast_to(mass - ALPHA * square, (count, LANES))

    lax.fori_loop(1, n_dev, wait_s, 0)

    def make_cost(k, _):
        pieces = [src_all[k * rep + i, 0:count, :] for i in range(rep)]
        masses = sum(src_all[k * rep + i, count : count + 1, :] for i in range(rep))
        loga[pl.ds(k, 1), :] = masses
        cost[k] = lax.dot_general(
            tcat[...], jnp.concatenate(pieces, axis=0), (((1,), (1,)), ((), ())),
            precision=lax.Precision.HIGHEST, preferred_element_type=jnp.float32)
        return 0

    lax.fori_loop(0, chunks, make_cost, 0)

    rows_at_once = min(nj, 128)

    def source_chunk(slot, k):
        pairs = []
        for r in range(0, nj, rows_at_once):
            x = cost[k, r : r + rows_at_once, :] + u[r : r + rows_at_once, :]
            x = x.reshape(rows_at_once // SUB, SUB, LANES)
            m = jnp.max(x, axis=0)
            pairs.append((m, jnp.sum(exp2(x - m[None]), axis=0)))
        m, s = lse_blocks(pairs)
        top = jnp.max(m, axis=0, keepdims=True)
        total = jnp.sum(s * exp2(m - top), axis=0, keepdims=True)
        part_lse[slot, p, pl.ds(k, 1), :] = top + log2(total)

    groups = math.gcd(nj // SUB, 8)

    def target_rows(i, _):
        for h in range(groups):
            rows = pl.ds(pl.multiple_of((i * groups + h) * SUB, SUB), SUB)
            pairs = []
            for k0 in range(0, chunks, 16):
                x = [cost[k, rows, :] + v[k : k + 1, :] for k in range(k0, min(k0 + 16, chunks))]
                m = functools.reduce(jnp.maximum, x)
                pairs.append((m, sum(exp2(y - m) for y in x)))
            m, s = lse_blocks(pairs)
            top = jnp.max(m, axis=1, keepdims=True)
            total = jnp.sum(s * exp2(m - top), axis=1, keepdims=True)
            u[rows, :] = logb[rows, :] - (top + log2(total))
        return 0

    def swap(slot, writer, other, sem_at):
        return pltpu.make_async_remote_copy(
            src_ref=part_lse.at[slot, p], dst_ref=part_lse.at[slot, writer],
            send_sem=x_send.at[slot, other], recv_sem=x_recv.at[slot, sem_at],
            device_id=(q * part + other, g), device_id_type=MESH)

    def iteration(t, _):
        slot = lax.rem(t, 2)

        def one(k, _):
            source_chunk(slot, k)
            return 0

        lax.fori_loop(0, chunks, one, 0)
        for step in range(1, part):
            other = lax.rem(p + step, part)
            swap(slot, p, other, p).start()
        for step in range(1, part):
            other = lax.rem(p + step, part)
            swap(slot, p, other, p).wait_send()
            swap(slot, other, other, other).wait_recv()
        parts = [part_lse[slot, i] for i in range(part)]
        top = functools.reduce(jnp.maximum, parts)
        v[...] = loga[...] - (top + log2(sum(exp2(y - top) for y in parts)))
        lax.fori_loop(0, nj // (SUB * groups), target_rows, 0)
        return 0

    lax.fori_loop(0, ITERS, iteration, 0)

    def to_lanes(column):
        return jnp.sum(jnp.where(eye, column, 0.0), axis=0, keepdims=True)

    src = src_ref[...]
    row = pl.ds(me // rep, 1)
    lse_s = loga[row, :] - v[row, :]
    first = to_lanes(jnp.sum(src * src, axis=1, keepdims=True)) - (1.0 / ALPHA) * lse_s
    tgt = tgt_ref[...]
    own = pl.ds(pl.multiple_of(mine_t * count, count), count)
    lse_t = logb[own, :] - u[own, :]
    second = to_lanes(jnp.sum(tgt * tgt, axis=1, keepdims=True) - (1.0 / ALPHA) * lse_t)
    picked = first[:, 0:count]
    for i in range(1, rep):
        picked = jnp.where(me % rep == i, first[:, i * count : (i + 1) * count], picked)
    out_ref[0:1, 0:count] = picked
    out_ref[1:2, 0:count] = second[:, 0:count]


def solution(mesh):
    blk_n, grp_n = mesh.shape["blk"], mesh.shape["grp"]
    n_dev = blk_n * grp_n

    def per_device(source, target, source_mass, target_mass):
        count, width = source.shape
        points = n_dev * count
        part = min(4, blk_n)
        while part < blk_n and (points // part) * points * 4 > BUDGET:
            part *= 2
        nj = points // part
        t_dev = n_dev // part
        chunks = points // LANES
        wide = count + SUB
        f32 = jnp.float32
        vmem = pl.BlockSpec(memory_space=pltpu.VMEM)
        dma = pltpu.SemaphoreType.DMA
        out = pl.pallas_call(
            functools.partial(kernel, blk_n, grp_n, part, count),
            out_shape=jax.ShapeDtypeStruct((2, count), f32),
            in_specs=[vmem] * 4,
            out_specs=vmem,
            scratch_shapes=[
                pltpu.VMEM((n_dev, wide, width), f32),
                pltpu.VMEM((t_dev, wide, width), f32),
                pltpu.VMEM((wide, width), f32),
                pltpu.VMEM((wide, width), f32),
                pltpu.VMEM((chunks, nj, LANES), f32),
                pltpu.VMEM((nj, width), f32),
                pltpu.VMEM((nj, LANES), f32),
                pltpu.VMEM((chunks, LANES), f32),
                pltpu.VMEM((chunks, LANES), f32),
                pltpu.VMEM((nj, LANES), f32),
                pltpu.VMEM((2, part, chunks, LANES), f32),
                dma((n_dev,)), dma((n_dev,)),
                dma((t_dev,)), dma((t_dev,)),
                dma((2, part)), dma((2, part)),
            ],
            compiler_params=pltpu.CompilerParams(
                collective_id=0, has_side_effects=True, vmem_limit_bytes=62 * 2**20),
        )(source, target, source_mass.reshape(1, count), target_mass.reshape(1, count))
        return out[0], out[1]

    both = P(("blk", "grp"))
    return jax.shard_map(
        per_device,
        mesh=mesh,
        in_specs=(P(("blk", "grp"), None), P(("blk", "grp"), None), both, both),
        out_specs=(both, both),
        check_vma=False,
    )
```

```python
import functools
import math

import jax
import jax.numpy as jnp
from jax import lax
from jax.experimental import pallas as pl
from jax.experimental.pallas import tpu as pltpu
from jax.sharding import PartitionSpec as P

ITERS = 8
eps = 0.5
LOG2E = math.log2(math.e)
ALPHA = LOG2E / eps
LANES = 128
SUB = 8
OCT = 8
MESH = pl.DeviceIdType.MESH
BUDGET = 36 * 2**20


def exp2(x):
    return jnp.exp2(x)


def log2(x):
    return jnp.log(x) * LOG2E


def lse_blocks(pairs):
    top = functools.reduce(jnp.maximum, [m for m, _ in pairs])
    if len(pairs) == 1:
        return pairs[0]
    return top, sum(s * exp2(m - top) for m, s in pairs)


def kernel(blk_n, grp_n, part, count, src_ref, tgt_ref, smass_ref, tmass_ref, out_ref,
           src_all, tgt_all, spack, tpack, cost, tcat, u, v, loga, logb, part_lse,
           s_send, f_send, s_recv, t_send, t_recv, x_send, x_recv):
    n_dev = blk_n * grp_n
    rep = LANES // count
    chunks = n_dev // rep
    quads = blk_n // part
    t_dev = quads * grp_n
    nj = t_dev * count
    b, g = lax.axis_index("blk"), lax.axis_index("grp")
    me = b * grp_n + g
    q, p = b // part, b % part
    mine_t = q * grp_n + g

    peers = n_dev // OCT
    z, low = (b // OCT) * grp_n + g, b % OCT

    def flip(i, bit):
        return i + bit * (1 - 2 * ((i // bit) % 2))

    def place(step, bits):
        peer = lax.rem(z + step, peers)
        home = low
        for bit in (1, 2, 4):
            if bits & bit:
                home = flip(home, bit)
        return ((peer // grp_n) * OCT + home) * grp_n + peer % grp_n

    barrier = pltpu.get_barrier_semaphore()

    def greet(step, _):
        other = place(step, 0)
        pl.semaphore_signal(barrier, inc=1, device_id=(other // grp_n, other % grp_n), device_id_type=MESH)
        return 0

    lax.fori_loop(1, peers, greet, 0)

    def greet_part(step, _):
        other = q * part + lax.rem(p + step, part)
        pl.semaphore_signal(barrier, inc=1, device_id=(other, g), device_id_type=MESH)
        return 0

    lax.fori_loop(1, part, greet_part, 0)

    lane = lax.broadcasted_iota(jnp.int32, (1, LANES), 1)
    here = lane // count == me % rep

    def pack(ref, mass_ref, out, scale):
        out[0:count, :] = ref[...] * scale
        row = log2(mass_ref[...])
        row = jnp.where(here, jnp.concatenate([row] * rep, axis=1), 0.0)
        out[count : count + SUB, :] = jnp.broadcast_to(row, (SUB, LANES))

    pack(src_ref, smass_ref, spack, 2.0 * ALPHA)
    pack(tgt_ref, tmass_ref, tpack, 1.0)
    src_all[pl.ds(me, 1)] = spack[...][None]
    tgt_all[pl.ds(mine_t, 1)] = tpack[...][None]
    pl.semaphore_wait(barrier, peers + part - 2)

    def tgt_copy(slot, r, sem_slot):
        return pltpu.make_async_remote_copy(
            src_ref=tpack, dst_ref=tgt_all.at[slot],
            send_sem=t_send.at[r], recv_sem=t_recv.at[sem_slot],
            device_id=((r // grp_n) * part + p, r % grp_n), device_id_type=MESH)

    def src_copy(slot, d, step):
        return pltpu.make_async_remote_copy(
            src_ref=spack, dst_ref=src_all.at[slot],
            send_sem=s_send.at[step], recv_sem=s_recv.at[slot],
            device_id=(d // grp_n, d % grp_n), device_id_type=MESH)

    def push(slot, way):
        return pltpu.make_async_remote_copy(
            src_ref=src_all.at[slot], dst_ref=src_all.at[slot],
            send_sem=f_send.at[way, slot], recv_sem=s_recv.at[slot],
            device_id=(flip(b, 2 ** way), g), device_id_type=MESH)

    def arrive(slot):
        src_copy(slot, me, 0).wait_recv()

    def send_t(step, _):
        tgt_copy(mine_t, lax.rem(mine_t + step, t_dev), mine_t).start()
        return 0

    def send_s(step, _):
        src_copy(me, place(step, 0), step).start()
        return 0

    def wait_t(step, _):
        r = lax.rem(mine_t + step, t_dev)
        tgt_copy(mine_t, r, mine_t).wait_send()
        tgt_copy(r, r, r).wait_recv()
        return 0

    def make_cost(k):
        pieces = [src_all[k * rep + i, 0:count, :] for i in range(rep)]
        masses = sum(src_all[k * rep + i, count : count + 1, :] for i in range(rep))
        loga[pl.ds(k, 1), :] = masses
        cost[k] = lax.dot_general(
            tcat[...], jnp.concatenate(pieces, axis=0), (((1,), (1,)), ((), ())),
            precision=lax.Precision.HIGHEST, preferred_element_type=jnp.float32)

    def costs(bits):
        home = low
        for bit in (1, 2, 4):
            if bits & bit:
                home = flip(home, bit)
        per = grp_n // rep

        def one(i, _):
            make_cost(((i // per) * OCT + home) * per + i % per)
            return 0

        lax.fori_loop(0, peers // rep, one, 0)

    for way in range(3):
        push(me, way).start()
    lax.fori_loop(1, peers, send_s, 0)
    lax.fori_loop(1, t_dev, send_t, 0)

    def relay(bits, ways):
        def go(step, _):
            slot = place(step, bits)
            arrive(slot)
            for way in ways:
                push(slot, way).start()
            return 0
        return go

    half = peers // 2
    lax.fori_loop(1, peers, relay(0, (1, 2, 0)), 0)
    lax.fori_loop(1, t_dev, wait_t, 0)

    eye = (lax.broadcasted_iota(jnp.int32, (count, LANES), 1) % count
           == lax.broadcasted_iota(jnp.int32, (count, LANES), 0))
    for r in range(t_dev):
        rows = slice(r * count, (r + 1) * count)
        block = tgt_all[r, 0:count, :]
        tcat[rows, :] = block
        mass = jnp.sum(jnp.where(eye, tgt_all[r, count : count + 1, :], 0.0), axis=1, keepdims=True)
        square = jnp.sum(block * block, axis=1, keepdims=True)
        logb[rows, :] = jnp.broadcast_to(mass, (count, LANES))
        u[rows, :] = jnp.broadcast_to(mass - ALPHA * square, (count, LANES))

    lax.fori_loop(0, half, relay(2, (2, 0)), 0)
    lax.fori_loop(0, half, relay(4, (0,)), 0)
    lax.fori_loop(half, peers, relay(4, (1, 0)), 0)
    lax.fori_loop(half, peers, relay(2, (0,)), 0)
    costs(0)
    costs(2)
    costs(4)
    lax.fori_loop(0, peers, relay(6, (0,)), 0)
    costs(6)
    for bits in (1, 3, 5, 7):
        lax.fori_loop(0, peers, relay(bits, ()), 0)
        costs(bits)

    def sent_s(step, _):
        src_copy(me, place(step, 0), step).wait_send()
        return 0

    def sent(bits, ways):
        def go(step, _):
            for way in ways:
                push(place(step, bits), way).wait_send()
            return 0
        return go

    lax.fori_loop(1, peers, sent_s, 0)
    lax.fori_loop(0, peers, sent(0, (0, 1, 2)), 0)
    lax.fori_loop(0, half, sent(2, (2, 0)), 0)
    lax.fori_loop(0, half, sent(4, (0,)), 0)
    lax.fori_loop(half, peers, sent(4, (1, 0)), 0)
    lax.fori_loop(half, peers, sent(2, (0,)), 0)
    lax.fori_loop(0, peers, sent(6, (0,)), 0)

    rows_at_once = min(nj, 128)

    def source_chunk(slot, k):
        pairs = []
        for r in range(0, nj, rows_at_once):
            x = cost[k, r : r + rows_at_once, :] + u[r : r + rows_at_once, :]
            x = x.reshape(rows_at_once // SUB, SUB, LANES)
            m = jnp.max(x, axis=0)
            pairs.append((m, jnp.sum(exp2(x - m[None]), axis=0)))
        m, s = lse_blocks(pairs)
        top = jnp.max(m, axis=0, keepdims=True)
        total = jnp.sum(s * exp2(m - top), axis=0, keepdims=True)
        part_lse[slot, p, pl.ds(k, 1), :] = top + log2(total)

    groups = math.gcd(nj // SUB, 8)

    def target_rows(i, _):
        for h in range(groups):
            rows = pl.ds(pl.multiple_of((i * groups + h) * SUB, SUB), SUB)
            pairs = []
            for k0 in range(0, chunks, 16):
                x = [cost[k, rows, :] + v[k : k + 1, :] for k in range(k0, min(k0 + 16, chunks))]
                m = functools.reduce(jnp.maximum, x)
                pairs.append((m, sum(exp2(y - m) for y in x)))
            m, s = lse_blocks(pairs)
            top = jnp.max(m, axis=1, keepdims=True)
            total = jnp.sum(s * exp2(m - top), axis=1, keepdims=True)
            u[rows, :] = logb[rows, :] - (top + log2(total))
        return 0

    def swap(slot, writer, other, sem_at):
        return pltpu.make_async_remote_copy(
            src_ref=part_lse.at[slot, p], dst_ref=part_lse.at[slot, writer],
            send_sem=x_send.at[slot, other], recv_sem=x_recv.at[slot, sem_at],
            device_id=(q * part + other, g), device_id_type=MESH)

    def iteration(t, _):
        slot = lax.rem(t, 2)

        def one(k, _):
            source_chunk(slot, k)
            return 0

        lax.fori_loop(0, chunks, one, 0)
        for step in range(1, part):
            other = lax.rem(p + step, part)
            swap(slot, p, other, p).start()
        for step in range(1, part):
            other = lax.rem(p + step, part)
            swap(slot, p, other, p).wait_send()
            swap(slot, other, other, other).wait_recv()
        parts = [part_lse[slot, i] for i in range(part)]
        top = functools.reduce(jnp.maximum, parts)
        v[...] = loga[...] - (top + log2(sum(exp2(y - top) for y in parts)))
        lax.fori_loop(0, nj // (SUB * groups), target_rows, 0)
        return 0

    lax.fori_loop(0, ITERS, iteration, 0)

    def to_lanes(column):
        return jnp.sum(jnp.where(eye, column, 0.0), axis=0, keepdims=True)

    src = src_ref[...]
    row = pl.ds(me // rep, 1)
    lse_s = loga[row, :] - v[row, :]
    first = to_lanes(jnp.sum(src * src, axis=1, keepdims=True)) - (1.0 / ALPHA) * lse_s
    tgt = tgt_ref[...]
    own = pl.ds(pl.multiple_of(mine_t * count, count), count)
    lse_t = logb[own, :] - u[own, :]
    second = to_lanes(jnp.sum(tgt * tgt, axis=1, keepdims=True) - (1.0 / ALPHA) * lse_t)
    picked = first[:, 0:count]
    for i in range(1, rep):
        picked = jnp.where(me % rep == i, first[:, i * count : (i + 1) * count], picked)
    out_ref[0:1, 0:count] = picked
    out_ref[1:2, 0:count] = second[:, 0:count]


def solution(mesh):
    blk_n, grp_n = mesh.shape["blk"], mesh.shape["grp"]
    n_dev = blk_n * grp_n

    def per_device(source, target, source_mass, target_mass):
        count, width = source.shape
        points = n_dev * count
        part = OCT
        while part < blk_n and (points // part) * points * 4 > BUDGET:
            part *= 2
        nj = points // part
        t_dev = n_dev // part
        chunks = points // LANES
        wide = count + SUB
        f32 = jnp.float32
        vmem = pl.BlockSpec(memory_space=pltpu.VMEM)
        dma = pltpu.SemaphoreType.DMA
        out = pl.pallas_call(
            functools.partial(kernel, blk_n, grp_n, part, count),
            out_shape=jax.ShapeDtypeStruct((2, count), f32),
            in_specs=[vmem] * 4,
            out_specs=vmem,
            scratch_shapes=[
                pltpu.VMEM((n_dev, wide, width), f32),
                pltpu.VMEM((t_dev, wide, width), f32),
                pltpu.VMEM((wide, width), f32),
                pltpu.VMEM((wide, width), f32),
                pltpu.VMEM((chunks, nj, LANES), f32),
                pltpu.VMEM((nj, width), f32),
                pltpu.VMEM((nj, LANES), f32),
                pltpu.VMEM((chunks, LANES), f32),
                pltpu.VMEM((chunks, LANES), f32),
                pltpu.VMEM((nj, LANES), f32),
                pltpu.VMEM((2, part, chunks, LANES), f32),
                dma((n_dev // OCT,)), dma((3, n_dev)), dma((n_dev,)),
                dma((t_dev,)), dma((t_dev,)),
                dma((2, part)), dma((2, part)),
            ],
            compiler_params=pltpu.CompilerParams(
                collective_id=0, has_side_effects=True, vmem_limit_bytes=62 * 2**20),
        )(source, target, source_mass.reshape(1, count), target_mass.reshape(1, count))
        return out[0], out[1]

    both = P(("blk", "grp"))
    return jax.shard_map(
        per_device,
        mesh=mesh,
        in_specs=(P(("blk", "grp"), None), P(("blk", "grp"), None), both, both),
        out_specs=(both, both),
        check_vma=False,
    )
```

```python
import functools
import math

import jax
import jax.numpy as jnp
from jax import lax
from jax.experimental import pallas as pl
from jax.experimental.pallas import tpu as pltpu
from jax.sharding import PartitionSpec as P

ITERS = 8
eps = 0.5
LOG2E = math.log2(math.e)
ALPHA = LOG2E / eps
LANES = 128
SUB = 8
OCT = 8
PIECES = 2
UNIT = 4
GROUPS = 32
MESH = pl.DeviceIdType.MESH
BUDGET = 36 * 2**20


def exp2(x):
    return jnp.exp2(x)


def log2(x):
    return jnp.log2(x)


def lse_blocks(pairs):
    top = functools.reduce(jnp.maximum, [m for m, _ in pairs])
    if len(pairs) == 1:
        return pairs[0]
    return top, sum(s * exp2(m - top) for m, s in pairs)


def kernel(blk_n, grp_n, part, count, pieces, src_ref, tgt_ref, smass_ref, tmass_ref, out_ref,
           src_all, tgt_all, spack, tpack, cost, tcat, u, v, loga, logb, part_lse, piece_top, piece_sum,
           s_send, f_send, s_recv, t_send, t_recv, x_send, x_recv):
    n_dev = blk_n * grp_n
    rep = LANES // count
    chunks = n_dev // rep
    quads = blk_n // part
    t_dev = quads * grp_n
    nj = t_dev * count
    b, g = lax.axis_index("blk"), lax.axis_index("grp")
    me = b * grp_n + g
    q, p = b // part, b % part
    mine_t = q * grp_n + g

    peers = n_dev // OCT
    z, low = (b // OCT) * grp_n + g, b % OCT

    def flip(i, bit):
        return i + bit * (1 - 2 * ((i // bit) % 2))

    def place(step, bits):
        peer = lax.rem(z + step, peers)
        home = low
        for bit in (1, 2, 4):
            if bits & bit:
                home = flip(home, bit)
        return ((peer // grp_n) * OCT + home) * grp_n + peer % grp_n

    barrier = pltpu.get_barrier_semaphore()

    def greet(step, _):
        other = place(step, 0)
        pl.semaphore_signal(barrier, inc=1, device_id=(other // grp_n, other % grp_n), device_id_type=MESH)
        return 0

    lax.fori_loop(1, peers, greet, 0)

    def greet_part(step, _):
        other = q * part + lax.rem(p + step, part)
        pl.semaphore_signal(barrier, inc=1, device_id=(other, g), device_id_type=MESH)
        return 0

    lax.fori_loop(1, part, greet_part, 0)

    lane = lax.broadcasted_iota(jnp.int32, (1, LANES), 1)
    here = lane // count == me % rep

    def pack(ref, mass_ref, out, scale):
        out[0:count, :] = ref[...] * scale
        row = log2(mass_ref[...])
        row = jnp.where(here, jnp.concatenate([row] * rep, axis=1), 0.0)
        out[count : count + SUB, :] = jnp.broadcast_to(row, (SUB, LANES))

    pack(src_ref, smass_ref, spack, 2.0 * ALPHA)
    pack(tgt_ref, tmass_ref, tpack, 1.0)
    src_all[pl.ds(me, 1)] = spack[...][None]
    tgt_all[pl.ds(mine_t, 1)] = tpack[...][None]
    pl.semaphore_wait(barrier, peers + part - 2)

    def tgt_copy(slot, r, sem_slot):
        return pltpu.make_async_remote_copy(
            src_ref=tpack, dst_ref=tgt_all.at[slot],
            send_sem=t_send.at[r], recv_sem=t_recv.at[sem_slot],
            device_id=((r // grp_n) * part + p, r % grp_n), device_id_type=MESH)

    def src_copy(slot, d, step):
        return pltpu.make_async_remote_copy(
            src_ref=spack, dst_ref=src_all.at[slot],
            send_sem=s_send.at[step], recv_sem=s_recv.at[slot],
            device_id=(d // grp_n, d % grp_n), device_id_type=MESH)

    def push(slot, way):
        return pltpu.make_async_remote_copy(
            src_ref=src_all.at[slot], dst_ref=src_all.at[slot],
            send_sem=f_send.at[way, slot], recv_sem=s_recv.at[slot],
            device_id=(flip(b, 2 ** way), g), device_id_type=MESH)

    def arrive(slot):
        src_copy(slot, me, 0).wait_recv()

    def send_t(step, _):
        tgt_copy(mine_t, lax.rem(mine_t + step, t_dev), mine_t).start()
        return 0

    def send_s(step, _):
        src_copy(me, place(step, 0), step).start()
        return 0

    def wait_t(step, _):
        r = lax.rem(mine_t + step, t_dev)
        tgt_copy(mine_t, r, mine_t).wait_send()
        tgt_copy(r, r, r).wait_recv()
        return 0

    def make_cost(k):
        blocks = [src_all[k * rep + i, 0:count, :] for i in range(rep)]
        masses = sum(src_all[k * rep + i, count : count + 1, :] for i in range(rep))
        loga[pl.ds(k, 1), :] = masses
        cost[k] = lax.dot_general(
            tcat[...], jnp.concatenate(blocks, axis=0), (((1,), (1,)), ((), ())),
            precision=lax.Precision.HIGHEST, preferred_element_type=jnp.float32)

    def costs(bits):
        home = low
        for bit in (1, 2, 4):
            if bits & bit:
                home = flip(home, bit)
        per = grp_n // rep

        def one(i, _):
            make_cost(((i // per) * OCT + home) * per + i % per)
            return 0

        lax.fori_loop(0, peers // rep, one, 0)

    for way in range(3):
        push(me, way).start()
    lax.fori_loop(1, peers, send_s, 0)
    lax.fori_loop(1, t_dev, send_t, 0)

    def relay(bits, ways):
        def go(step, _):
            slot = place(step, bits)
            arrive(slot)
            for way in ways:
                push(slot, way).start()
            return 0
        return go

    half = peers // 2
    lax.fori_loop(1, peers, relay(0, (1, 2, 0)), 0)
    lax.fori_loop(1, t_dev, wait_t, 0)

    eye = (lax.broadcasted_iota(jnp.int32, (count, LANES), 1) % count
           == lax.broadcasted_iota(jnp.int32, (count, LANES), 0))
    for r in range(t_dev):
        rows = slice(r * count, (r + 1) * count)
        block = tgt_all[r, 0:count, :]
        tcat[rows, :] = block
        mass = jnp.sum(jnp.where(eye, tgt_all[r, count : count + 1, :], 0.0), axis=1, keepdims=True)
        square = jnp.sum(block * block, axis=1, keepdims=True)
        logb[rows, :] = jnp.broadcast_to(mass, (count, LANES))
        u[rows, :] = jnp.broadcast_to(mass - ALPHA * square, (count, LANES))

    lax.fori_loop(0, half, relay(2, (2, 0)), 0)
    lax.fori_loop(0, half, relay(4, (0,)), 0)
    lax.fori_loop(half, peers, relay(4, (1, 0)), 0)
    lax.fori_loop(half, peers, relay(2, (0,)), 0)
    costs(0)
    costs(2)
    costs(4)
    lax.fori_loop(0, peers, relay(6, (0,)), 0)
    costs(6)
    for bits in (1, 3, 5, 7):
        lax.fori_loop(0, peers, relay(bits, ()), 0)
        costs(bits)

    def sent_s(step, _):
        src_copy(me, place(step, 0), step).wait_send()
        return 0

    def sent(bits, ways):
        def go(step, _):
            for way in ways:
                push(place(step, bits), way).wait_send()
            return 0
        return go

    lax.fori_loop(1, peers, sent_s, 0)
    lax.fori_loop(0, peers, sent(0, (0, 1, 2)), 0)
    lax.fori_loop(0, half, sent(2, (2, 0)), 0)
    lax.fori_loop(0, half, sent(4, (0,)), 0)
    lax.fori_loop(half, peers, sent(4, (1, 0)), 0)
    lax.fori_loop(half, peers, sent(2, (0,)), 0)
    lax.fori_loop(0, peers, sent(6, (0,)), 0)

    rows_at_once = min(nj, 128)
    size = chunks // pieces
    unit = math.gcd(size, UNIT)

    def source_unit(slot, c, k0):
        tops, totals = [], []
        for h in range(unit):
            pairs = []
            for r in range(0, nj, rows_at_once):
                x = cost[c * size + k0 + h, r : r + rows_at_once, :] + u[r : r + rows_at_once, :]
                x = x.reshape(rows_at_once // SUB, SUB, LANES)
                m = jnp.max(x, axis=0)
                pairs.append((m, jnp.sum(exp2(x - m[None]), axis=0)))
            m, s = lse_blocks(pairs)
            top = jnp.max(m, axis=0, keepdims=True)
            tops.append(top)
            totals.append(jnp.sum(s * exp2(m - top), axis=0, keepdims=True))
        part_lse[slot, c, p, pl.ds(k0, unit), :] = (
            jnp.concatenate(tops, axis=0) + log2(jnp.concatenate(totals, axis=0)))

    groups = math.gcd(nj // SUB, GROUPS)

    def target_rows(c, i):
        for h in range(groups):
            rows = pl.ds(pl.multiple_of((i * groups + h) * SUB, SUB), SUB)
            pairs = []
            for k0 in range(c * size, (c + 1) * size, 16):
                x = [cost[k, rows, :] + v[k : k + 1, :] for k in range(k0, min(k0 + 16, (c + 1) * size))]
                m = functools.reduce(jnp.maximum, x)
                pairs.append((m, sum(exp2(y - m) for y in x)))
            m, s = lse_blocks(pairs)
            if c < pieces - 1:
                piece_top[c, rows, :] = m
                piece_sum[c, rows, :] = s
                continue
            m, s = lse_blocks([(m, s)] + [(piece_top[i2, rows, :], piece_sum[i2, rows, :]) for i2 in range(c)])
            top = jnp.max(m, axis=1, keepdims=True)
            total = jnp.sum(s * exp2(m - top), axis=1, keepdims=True)
            u[rows, :] = logb[rows, :] - (top + log2(total))

    def swap(slot, c, writer, other, sem_at):
        return pltpu.make_async_remote_copy(
            src_ref=part_lse.at[slot, c, p], dst_ref=part_lse.at[slot, c, writer],
            send_sem=x_send.at[slot, c, other], recv_sem=x_recv.at[slot, c, sem_at],
            device_id=(q * part + other, g), device_id_type=MESH)

    def iteration(t, _):
        slot = lax.rem(t, 2)

        for c in range(pieces):
            def one(i, _):
                source_unit(slot, c, i * unit)
                return 0

            if size == unit:
                source_unit(slot, c, 0)
            else:
                lax.fori_loop(0, size // unit, one, 0)
            for step in range(1, part):
                swap(slot, c, p, lax.rem(p + step, part), p).start()
        for c in range(pieces):
            for step in range(1, part):
                other = lax.rem(p + step, part)
                swap(slot, c, other, other, other).wait_recv()
            parts = [part_lse[slot, c, i] for i in range(part)]
            top = functools.reduce(jnp.maximum, parts)
            rows = slice(c * size, (c + 1) * size)
            v[rows, :] = loga[rows, :] - (top + log2(sum(exp2(y - top) for y in parts)))

            def two(i, _):
                target_rows(c, i)
                return 0

            lax.fori_loop(0, nj // (SUB * groups), two, 0)
        for c in range(pieces):
            for step in range(1, part):
                swap(slot, c, p, lax.rem(p + step, part), p).wait_send()
        return 0

    lax.fori_loop(0, ITERS, iteration, 0)

    def to_lanes(column):
        return jnp.sum(jnp.where(eye, column, 0.0), axis=0, keepdims=True)

    src = src_ref[...]
    row = pl.ds(me // rep, 1)
    lse_s = loga[row, :] - v[row, :]
    first = to_lanes(jnp.sum(src * src, axis=1, keepdims=True)) - (1.0 / ALPHA) * lse_s
    tgt = tgt_ref[...]
    own = pl.ds(pl.multiple_of(mine_t * count, count), count)
    lse_t = logb[own, :] - u[own, :]
    second = to_lanes(jnp.sum(tgt * tgt, axis=1, keepdims=True) - (1.0 / ALPHA) * lse_t)
    picked = first[:, 0:count]
    for i in range(1, rep):
        picked = jnp.where(me % rep == i, first[:, i * count : (i + 1) * count], picked)
    out_ref[0:1, 0:count] = picked
    out_ref[1:2, 0:count] = second[:, 0:count]


def solution(mesh):
    blk_n, grp_n = mesh.shape["blk"], mesh.shape["grp"]
    n_dev = blk_n * grp_n

    def per_device(source, target, source_mass, target_mass):
        count, width = source.shape
        points = n_dev * count
        part = OCT
        while part < blk_n and (points // part) * points * 4 > BUDGET:
            part *= 2
        nj = points // part
        t_dev = n_dev // part
        chunks = points // LANES
        pieces = math.gcd(chunks, PIECES)
        wide = count + SUB
        f32 = jnp.float32
        vmem = pl.BlockSpec(memory_space=pltpu.VMEM)
        dma = pltpu.SemaphoreType.DMA
        out = pl.pallas_call(
            functools.partial(kernel, blk_n, grp_n, part, count, pieces),
            out_shape=jax.ShapeDtypeStruct((2, count), f32),
            in_specs=[vmem] * 4,
            out_specs=vmem,
            scratch_shapes=[
                pltpu.VMEM((n_dev, wide, width), f32),
                pltpu.VMEM((t_dev, wide, width), f32),
                pltpu.VMEM((wide, width), f32),
                pltpu.VMEM((wide, width), f32),
                pltpu.VMEM((chunks, nj, LANES), f32),
                pltpu.VMEM((nj, width), f32),
                pltpu.VMEM((nj, LANES), f32),
                pltpu.VMEM((chunks, LANES), f32),
                pltpu.VMEM((chunks, LANES), f32),
                pltpu.VMEM((nj, LANES), f32),
                pltpu.VMEM((2, pieces, part, chunks // pieces, LANES), f32),
                pltpu.VMEM((pieces, nj, LANES), f32),
                pltpu.VMEM((pieces, nj, LANES), f32),
                dma((n_dev // OCT,)), dma((3, n_dev)), dma((n_dev,)),
                dma((t_dev,)), dma((t_dev,)),
                dma((2, pieces, part)), dma((2, pieces, part)),
            ],
            compiler_params=pltpu.CompilerParams(
                collective_id=0, has_side_effects=True, vmem_limit_bytes=62 * 2**20),
        )(source, target, source_mass.reshape(1, count), target_mass.reshape(1, count))
        return out[0], out[1]

    both = P(("blk", "grp"))
    return jax.shard_map(
        per_device,
        mesh=mesh,
        in_specs=(P(("blk", "grp"), None), P(("blk", "grp"), None), both, both),
        out_specs=(both, both),
        check_vma=False,
    )
```
